32 devices in a mesh: dp: 4 (over y, z), tp: 8 (over x, core).
Axes of the slice: x: 4, y: 2, z: 2, core: 2. Of those that a mesh axis runs over, the one named last changes fastest.
The devices are a block of a 4x4x8 slice.
Arguments:
- x: bfloat16 [12288, 2048], P(('dp', 'tp')), parts along dimension 0
- dy: bfloat16 [12288, 2048], P(('dp', 'tp')), parts along dimension 0
- wg: bfloat16 [2048, 8192], P(None, 'tp')
- wu: bfloat16 [2048, 8192], P(None, 'tp')
- wd: bfloat16 [8192, 2048], P('tp')
- ug: bfloat16 [12288, 8192], P('dp', 'tp'), parts along dimension 0
- uu: bfloat16 [12288, 8192], P('dp', 'tp'), parts along dimension 0
Outputs:
- output 1: bfloat16 [12288, 2048], P(('dp', 'tp')), parts along dimension 0
- output 2: float32 [8192, 8192], P('dp', 'tp'), parts along dimension 0
- output 3: float32 [8192, 8192], P('dp', 'tp'), parts along dimension 0
- output 4: float32 [32768, 2048], P(('dp', 'tp')), parts along dimension 0
There are 4 independent parts. The reference program is written for one: setup_inputs(seed, part) draws one part's arguments, and reference() takes and returns one part's arrays. A program takes and returns all parts, laid end to end along the dimension named above; an argument that names none is the same for every part.
All inputs are finite; a program needn't handle non-finite values.
Results may differ from the reference program's by a relative error of at most 0.0130648.
Values are sent between devices in bfloat16 or wider.
A program may use at most 768 MiB of HBM per device.

```python
import jax
import jax.numpy as jnp

T = 3072
H = 2048
F = 8192


def setup_inputs(seed: int = 0, part: int = 0) -> dict:
    key = jax.random.key(seed)
    k_shared, k_part = jax.random.split(key)
    kg, ku, kd = jax.random.split(k_shared, 3)
    kx, kdy, kug, kuu = jax.random.split(jax.random.fold_in(k_part, part), 4)
    wg = (jax.random.normal(kg, (H, F), jnp.float32) * H ** -0.5).astype(jnp.bfloat16)
    wu = (jax.random.normal(ku, (H, F), jnp.float32) * H ** -0.5).astype(jnp.bfloat16)
    wd = (jax.random.normal(kd, (F, H), jnp.float32) * F ** -0.5).astype(jnp.bfloat16)
    x = jax.random.normal(kx, (T, H), jnp.float32).astype(jnp.bfloat16)
    dy = jax.random.normal(kdy, (T, H), jnp.float32).astype(jnp.bfloat16)
    ug = jax.random.normal(kug, (T, F), jnp.float32).astype(jnp.bfloat16)
    uu = jax.random.normal(kuu, (T, F), jnp.float32).astype(jnp.bfloat16)
    return {"x": x, "dy": dy, "wg": wg, "wu": wu, "wd": wd, "ug": ug, "uu": uu}


def reference(x, dy, wg, wu, wd, ug, uu):
    ug32 = ug.astype(jnp.float32)
    uu32 = uu.astype(jnp.float32)
    s = jax.nn.sigmoid(ug32)
    a = ug32 * s
    z = (a * uu32).astype(jnp.bfloat16)
    dwd = jnp.dot(z.T, dy, preferred_element_type=jnp.float32)
    g = jnp.dot(dy, wd.T, preferred_element_type=jnp.float32)
    duu = (g * a).astype(jnp.bfloat16)
    dug = (g * uu32 * s * (1.0 + ug32 * (1.0 - s))).astype(jnp.bfloat16)
    p = jnp.dot(dug, wg.T, preferred_element_type=jnp.float32) + jnp.dot(duu, wu.T, preferred_element_type=jnp.float32)
    dx = p.astype(jnp.bfloat16)
    dwg = jnp.dot(x.T, dug, preferred_element_type=jnp.float32)
    dwu = jnp.dot(x.T, duu, preferred_element_type=jnp.float32)
    return (dx, dwg, dwu, dwd)
```

```python
import functools

import jax
import jax.numpy as jnp
from jax import lax
from jax.experimental import pallas as pl
from jax.experimental.pallas import tpu as pltpu
from jax.sharding import PartitionSpec as P


MESH = pl.DeviceIdType.MESH
BF = jnp.bfloat16
F32 = jnp.float32
NT = (((1,), (1,)), ((), ()))
TN = (((0,), (0,)), ((), ()))

R_A, R_B, L_A, L_B, F_R, F_L, Q_OWN, Q_LA, Q_LB, Q_RA, Q_RB, Q_OA, Q_OB = range(13)


def gather_kernel(
    n, x, dy, wd, wg, wu, ug, uu,
    xg, dyg, dug, duu, dwd, s_own, s_la, s_lb, s_ra, s_rb, s_oa, s_ob, pbuf, rbuf,
    vwd, vwg, vwu, vdy, vug, vuu, vdug, vduu, vz, vp, vq, vdw,
    ss, rs, sx, rx, wsem, usem, dsem, osem, psem, qsem,
):
    rows, hid = x.shape
    half = rows // 2
    ff = wd.shape[0]
    me = lax.axis_index("tp")
    core = lax.rem(me, 2)
    right, left = lax.rem(me + 2, n), lax.rem(me + n - 2, n)
    opp = lax.rem(me + 4, n)
    mate = me + 1 - 2 * core

    def whole(d):
        return pl.ds(pl.multiple_of(d * rows, rows), rows)

    def part(d, h):
        return pl.ds(pl.multiple_of(d * rows + h * half, half), half)

    def at(slot):
        return pl.ds(slot * rows, rows)

    def mate_of(d):
        return d + 1 - 2 * core

    def remote(src, dst, k, i, dev):
        return pltpu.make_async_remote_copy(
            src, dst, ss.at[k, i], rs.at[k, i], device_id={"tp": dev}, device_id_type=MESH
        )

    gathers = ((dy, dyg), (x, xg))

    def send_own(k):
        src, dst = gathers[k]
        a, b = pl.ds(0, half), pl.ds(half, half)
        remote(src.at[a], dst.at[part(me, 0)], k, R_A, right).start()
        remote(src.at[b], dst.at[part(me, 1)], k, L_B, left).start()
        remote(src, dst.at[whole(me)], k, Q_OWN, mate).start()
        remote(src.at[b], dst.at[part(me, 1)], k, R_B, right).start()
        remote(src.at[a], dst.at[part(me, 0)], k, L_A, left).start()

    def piece(k, d, h, i, dev):
        dst = gathers[k][1]
        return remote(dst.at[part(d, h)], dst.at[part(d, h)], k, i, dev)

    def relay_first(k):
        piece(k, left, 0, R_A, right).wait_recv()
        piece(k, left, 0, F_R, right).start()
        piece(k, left, 0, Q_LA, mate).start()
        piece(k, right, 1, L_B, left).wait_recv()
        piece(k, right, 1, F_L, left).start()
        piece(k, right, 1, Q_RB, mate).start()

    def relay_second(k):
        piece(k, left, 1, R_B, right).wait_recv()
        piece(k, left, 1, Q_LB, mate).start()
        piece(k, right, 0, L_A, left).wait_recv()
        piece(k, right, 0, Q_RA, mate).start()

    def relay_third(k):
        piece(k, opp, 0, F_R, right).wait_recv()
        piece(k, opp, 0, Q_OA, mate).start()
        piece(k, opp, 1, F_L, left).wait_recv()
        piece(k, opp, 1, Q_OB, mate).start()

    def drain(k):
        src, dst = gathers[k]
        for i in (R_A, R_B, L_A, L_B, F_R, F_L, Q_LA, Q_LB, Q_RA, Q_RB, Q_OA, Q_OB):
            piece(k, me, 0, i, right).wait_send()
        remote(src, dst.at[whole(me)], k, Q_OWN, mate).wait_send()

    def wait_mate(k, *slots):
        for i in slots:
            piece(k, me, 0, i, mate).wait_recv()

    barrier = pltpu.get_barrier_semaphore()
    for dev in (right, left, mate):
        pl.semaphore_signal(barrier, inc=1, device_id={"tp": dev}, device_id_type=MESH)
    pl.semaphore_wait(barrier, 3)

    send_own(0)
    loads = [pltpu.make_async_copy(a, b, wsem.at[i]) for i, (a, b) in enumerate(((wd, vwd), (wg, vwg), (wu, vwu)))]
    for c in loads:
        c.start()

    def u_load(d, slot):
        return (
            pltpu.make_async_copy(ug.at[whole(d)], vug.at[slot], usem.at[0, slot]),
            pltpu.make_async_copy(uu.at[whole(d)], vuu.at[slot], usem.at[1, slot]),
        )

    def outs(d, slot):
        return (
            pltpu.make_async_copy(vdug.at[slot], dug.at[whole(d)], osem.at[0, slot]),
            pltpu.make_async_copy(vduu.at[slot], duu.at[whole(d)], osem.at[1, slot]),
        )

    def p_out(slot, j):
        if slot == 0:
            return (pltpu.make_async_copy(vp.at[0], pbuf.at[j], psem.at[0]),)
        if j == 0:
            return (pltpu.make_async_copy(vp.at[1], s_own, psem.at[1]),)
        a, b = ((s_la, s_lb), (s_ra, s_rb), (s_oa, s_ob))[j - 1]
        return (
            pltpu.make_async_copy(vp.at[1, pl.ds(0, half)], a, psem.at[1]),
            pltpu.make_async_copy(vp.at[1, pl.ds(half, half)], b, psem.at[2]),
        )

    def swap(j):
        return pltpu.make_async_remote_copy(
            pbuf.at[j], rbuf.at[j], sx.at[j], rx.at[j], device_id={"tp": mate}, device_id_type=MESH
        )

    chips = (me, left, right, opp)
    order = [(j, slot, mate_of(chips[j]) if slot == 0 else chips[j]) for j in range(4) for slot in (0, 1)]

    for c in u_load(order[0][2], 0):
        c.start()
    own_x = (pltpu.make_async_copy(x, vq, qsem.at[1]), pltpu.make_async_copy(vq, xg.at[whole(me)], qsem.at[1]))
    own_dy = (pltpu.make_async_copy(dy, vdy.at[at(1)], dsem.at[1]), pltpu.make_async_copy(vdy.at[at(1)], dyg.at[whole(me)], qsem.at[2]))
    own_x[0].start()
    own_dy[0].start()
    own_x[0].wait()
    own_x[1].start()
    own_dy[0].wait()
    own_dy[1].start()
    own_x[1].wait()

    gn = min(256, ff)
    hn = min(512, hid)

    def block(step):
        j, slot, d = order[step]
        if step != 1:
            load = pltpu.make_async_copy(dyg.at[whole(d)], vdy.at[at(slot)], dsem.at[slot])
            load.start()
            load.wait()
        for c in u_load(d, slot):
            c.wait()
        if step + 1 < 8:
            for c in u_load(order[step + 1][2], 1 - slot):
                c.start()
        if step >= 2:
            for c in outs(d, slot):
                c.wait()
        if slot == 1:
            for c in p_out(0, j):
                c.wait()
            swap(j).start()

        @pl.loop(0, ff // gn)
        def _(i):
            cols = pl.ds(pl.multiple_of(i * gn, gn), gn)
            g = lax.dot_general(vdy[at(slot), :], vwd[cols, :], NT, preferred_element_type=F32)
            u = vug[slot, :, cols].astype(F32)
            v = vuu[slot, :, cols].astype(F32)
            s = jax.nn.sigmoid(u)
            a = u * s
            vz[at(slot), cols] = (a * v).astype(BF)
            vduu[slot, :, cols] = (g * a).astype(BF)
            vdug[slot, :, cols] = (g * v * s * (1.0 + u * (1.0 - s))).astype(BF)

        for c in outs(d, slot):
            c.start()
        if slot == 1:
            swap(j).wait_recv()
            got = pltpu.make_async_copy(rbuf.at[j], vq, qsem.at[0])
            got.start()
            got.wait()
            if j > 0:
                for c in p_out(1, j - 1):
                    c.wait()

        @pl.loop(0, hid // hn)
        def _(i):
            cols = pl.ds(pl.multiple_of(i * hn, hn), hn)
            p = lax.dot_general(vdug[slot], vwg[cols, :], NT, preferred_element_type=F32)
            p += lax.dot_general(vduu[slot], vwu[cols, :], NT, preferred_element_type=F32)
            if slot == 1:
                p += vq[:, cols].astype(F32)
            vp[slot, :, cols] = p.astype(BF)

        for c in p_out(slot, j):
            c.start()
        if slot == 1:
            nt = min(512, hid)

            @pl.loop(0, ff // gn)
            def _(i):
                mine = pl.ds(pl.multiple_of(i * gn, gn), gn)
                zt = vz[:, mine]
                for k in range(0, hid, nt):
                    part_sum = lax.dot_general(zt, vdy[:, k : k + nt], TN, preferred_element_type=F32)
                    if j == 0:
                        vdw[mine, k : k + nt] = part_sum
                    else:
                        vdw[mine, k : k + nt] += part_sum

    remote(dy, dyg.at[whole(me)], 0, Q_OWN, mate).wait_recv()
    for c in loads:
        c.wait()
    block(0)
    block(1)
    own_dy[1].wait()
    relay_first(0)
    send_own(1)
    relay_second(0)
    wait_mate(0, Q_LA, Q_LB)
    block(2)
    block(3)
    wait_mate(0, Q_RA, Q_RB)
    relay_third(0)
    block(4)
    block(5)
    wait_mate(0, Q_OA, Q_OB)
    relay_first(1)
    block(6)
    block(7)
    dw_out = pltpu.make_async_copy(vdw, dwd, qsem.at[1])
    dw_out.start()
    relay_second(1)
    for step in (6, 7):
        j, slot, d = order[step]
        for c in outs(d, slot):
            c.wait()
    for c in p_out(1, 3):
        c.wait()
    for j in range(4):
        swap(j).wait_send()
    relay_third(1)
    dw_out.wait()
    remote(x, xg.at[whole(me)], 1, Q_OWN, mate).wait_recv()
    wait_mate(1, Q_LA, Q_LB, Q_RA, Q_RB, Q_OA, Q_OB)
    drain(0)
    drain(1)


def gather_and_local(n, x, dy, wd, wg, wu, ug, uu):
    rows, hid = x.shape
    tok, ff = ug.shape
    half = rows // 2
    any_ = pl.BlockSpec(memory_space=pl.ANY)
    sds = jax.ShapeDtypeStruct
    out = [sds((tok, hid), BF)] * 2 + [sds((tok, ff), BF)] * 2 + [sds((ff, hid), F32), sds((rows, hid), BF)] + [sds((half, hid), BF)] * 6
    out += [sds((n // 2, rows, hid), BF)] * 2
    return pl.pallas_call(
        functools.partial(gather_kernel, n),
        out_shape=out,
        in_specs=[any_] * 7,
        out_specs=[any_] * len(out),
        scratch_shapes=[
            pltpu.VMEM(wd.shape, BF), pltpu.VMEM(wg.shape, BF), pltpu.VMEM(wu.shape, BF),
            pltpu.VMEM((2 * rows, hid), BF),
            pltpu.VMEM((2, rows, ff), BF), pltpu.VMEM((2, rows, ff), BF),
            pltpu.VMEM((2, rows, ff), BF), pltpu.VMEM((2, rows, ff), BF), pltpu.VMEM((2 * rows, ff), BF),
            pltpu.VMEM((2, rows, hid), BF),
            pltpu.VMEM((rows, hid), BF),
            pltpu.VMEM((ff, hid), F32),
            pltpu.SemaphoreType.DMA((2, 13)), pltpu.SemaphoreType.DMA((2, 13)),
            pltpu.SemaphoreType.DMA((4,)), pltpu.SemaphoreType.DMA((4,)),
            pltpu.SemaphoreType.DMA((3,)), pltpu.SemaphoreType.DMA((2, 2)), pltpu.SemaphoreType.DMA((2,)),
            pltpu.SemaphoreType.DMA((2, 2)), pltpu.SemaphoreType.DMA((3,)), pltpu.SemaphoreType.DMA((3,)),
        ],
        compiler_params=pltpu.CompilerParams(collective_id=0, has_side_effects=True, vmem_limit_bytes=60 * 2**20),
        cost_estimate=pl.CostEstimate(flops=8 * tok * hid * ff, bytes_accessed=100 * 2**20, transcendentals=tok * ff),
    )(x, dy, wd, wg, wu, ug, uu)


def tokens_kernel(kt, a, b, o, vb, sem):
    tok = a.shape[0]
    copies = [
        pltpu.make_async_copy(b.at[pl.ds(k, kt)], vb.at[pl.ds(k, kt)], sem.at[k // kt]) for k in range(0, tok, kt)
    ]

    @pl.when(pl.program_id(0) == 0)
    def _():
        for c in copies:
            c.start()
        for i, c in enumerate(copies):
            c.wait()
            ks = pl.ds(i * kt, kt)
            p = lax.dot_general(a[ks, :], vb[ks, :], TN, preferred_element_type=F32)
            if i == 0:
                o[...] = p
            else:
                o[...] += p

    @pl.when(pl.program_id(0) > 0)
    def _():
        o[...] = lax.dot_general(a[...], vb[...], TN, preferred_element_type=F32)


def over_tokens(a, b, m_tile=256, kt=768):
    tok, m = a.shape
    k = b.shape[1]
    m_tile, kt = min(m_tile, m), min(kt, tok)
    return pl.pallas_call(
        functools.partial(tokens_kernel, kt),
        grid=(m // m_tile,),
        out_shape=jax.ShapeDtypeStruct((m, k), F32),
        in_specs=[pl.BlockSpec((tok, m_tile), lambda i: (0, i)), pl.BlockSpec(memory_space=pl.ANY)],
        out_specs=pl.BlockSpec((m_tile, k), lambda i: (i, 0)),
        scratch_shapes=[pltpu.VMEM((tok, k), BF), pltpu.SemaphoreType.DMA((tok // kt,))],
        compiler_params=pltpu.CompilerParams(vmem_limit_bytes=62 * 2**20),
        cost_estimate=pl.CostEstimate(
            flops=2 * tok * m * k, bytes_accessed=2 * tok * (m + k) + 4 * m * k, transcendentals=0
        ),
    )(a, b)


def sum_kernel(*refs):
    for i, group in enumerate((refs[1:3], refs[3:5])):
        total = refs[0][i].astype(F32)
        for r in group:
            total += r[...].astype(F32)
        refs[-1][i] = total.astype(BF)


def final_sum(own, a_terms, b_terms, steps=4):
    rows, hid = own.shape
    half = rows // 2
    t = half // steps
    both = pl.BlockSpec((2, t, hid), lambda i: (0, i, 0))
    one = pl.BlockSpec((t, hid), lambda i: (i, 0))
    return pl.pallas_call(
        sum_kernel,
        grid=(steps,),
        out_shape=jax.ShapeDtypeStruct((2, half, hid), BF),
        in_specs=[both] + [one] * 4,
        out_specs=both,
        compiler_params=pltpu.CompilerParams(vmem_limit_bytes=16 * 2**20),
        cost_estimate=pl.CostEstimate(flops=rows * hid * 3, bytes_accessed=8 * rows * hid, transcendentals=0),
    )(own.reshape(2, half, hid), *a_terms, *b_terms).reshape(rows, hid)


def solution(mesh):
    tok = P(("dp", "tp"), None)
    col = P(None, "tp")
    row = P("tp", None)
    act = P("dp", "tp")
    n = mesh.shape["tp"]
    to_right = [(i, (i + 2) % n) for i in range(n)]
    to_left = [(i, (i - 2) % n) for i in range(n)]

    def add(*terms):
        return functools.reduce(jnp.add, [t.astype(F32) for t in terms]).astype(BF)

    def body(x, dy, wg, wu, wd, ug, uu):
        xg, _, dug, duu, dwd, s_own, s_la, s_lb, s_ra, s_rb, s_oa, s_ob, _, _ = gather_and_local(
            n, x, dy, wd, wg, wu, ug, uu
        )

        def right(v):
            return lax.ppermute(v, "tp", to_right)

        def left(v):
            return lax.ppermute(v, "tp", to_left)

        from_right = left(s_oa)
        from_left = right(s_ob)
        direct_a = right(s_ra)
        direct_b = left(s_lb)
        dwg = over_tokens(xg, dug)
        from_right, from_left, dwg = lax.optimization_barrier((from_right, from_left, dwg))
        next_l = add(s_la, from_right)
        next_r = add(s_rb, from_left)
        next_l, next_r, xg = lax.optimization_barrier((next_l, next_r, xg))
        relay_a = left(next_l)
        relay_b = right(next_r)
        dwu = over_tokens(xg, duu)
        dx = final_sum(s_own, (direct_a, relay_a), (direct_b, relay_b))
        return dx, dwg, dwu, dwd

    return jax.shard_map(
        body, mesh=mesh, in_specs=(tok, tok, col, col, row, act, act), out_specs=(tok, act, act, tok), check_vma=False
    )
```

```python
import functools

import jax
import jax.numpy as jnp
from jax import lax
from jax.experimental import pallas as pl
from jax.experimental.pallas import tpu as pltpu
from jax.sharding import PartitionSpec as P


MESH = pl.DeviceIdType.MESH
BF = jnp.bfloat16
F32 = jnp.float32
NT = (((1,), (1,)), ((), ()))
TN = (((0,), (0,)), ((), ()))

EARLY = 3

R_A, R_B, L_A, L_B, F_R, F_L, Q_OWN, Q_LA, Q_LB, Q_RA, Q_RB, Q_OA, Q_OB = range(13)


def gather_kernel(
    n, x, dy, wd, wg, wu, ug, uu,
    xg, dyg, dug, duu, dwd, s_own, s_la, s_lb0, s_lb, s_ra0, s_ra, s_rb, s_oa, s_ob, got_a, got_b,
    vwd, vwg, vwu, vdy, vug, vuu, vdug, vduu, vz, vp, vq, vdw,
    ss, rs, sx, rx, se, re, wsem, usem, dsem, osem, psem, qsem,
):
    rows, hid = x.shape
    half = rows // 2
    ff = wd.shape[0]
    me = lax.axis_index("tp")
    core = lax.rem(me, 2)
    right, left = lax.rem(me + 2, n), lax.rem(me + n - 2, n)
    opp = lax.rem(me + 4, n)
    mate = me + 1 - 2 * core

    def whole(d):
        return pl.ds(pl.multiple_of(d * rows, rows), rows)

    def part(d, h):
        return pl.ds(pl.multiple_of(d * rows + h * half, half), half)

    def at(slot):
        return pl.ds(slot * rows, rows)

    def send(src, dst, s_sem, r_sem, dev):
        return pltpu.make_async_remote_copy(
            src, dst, s_sem, r_sem, device_id={"tp": dev}, device_id_type=MESH
        )

    def remote(src, dst, k, i, dev):
        return send(src, dst, ss.at[k, i], rs.at[k, i], dev)

    gathers = ((dy, dyg), (x, xg))

    def send_own(k):
        src, dst = gathers[k]
        a, b = pl.ds(0, half), pl.ds(half, half)
        remote(src.at[a], dst.at[part(me, 0)], k, R_A, right).start()
        remote(src.at[b], dst.at[part(me, 1)], k, L_B, left).start()
        remote(src, dst.at[whole(me)], k, Q_OWN, mate).start()
        remote(src.at[b], dst.at[part(me, 1)], k, R_B, right).start()
        remote(src.at[a], dst.at[part(me, 0)], k, L_A, left).start()

    def piece(k, d, h, i, dev):
        dst = gathers[k][1]
        return remote(dst.at[part(d, h)], dst.at[part(d, h)], k, i, dev)

    def relay_first(k):
        piece(k, left, 0, R_A, right).wait_recv()
        piece(k, left, 0, F_R, right).start()
        piece(k, left, 0, Q_LA, mate).start()
        piece(k, right, 1, L_B, left).wait_recv()
        piece(k, right, 1, F_L, left).start()
        piece(k, right, 1, Q_RB, mate).start()

    def relay_second(k):
        piece(k, left, 1, R_B, right).wait_recv()
        piece(k, left, 1, Q_LB, mate).start()
        piece(k, right, 0, L_A, left).wait_recv()
        piece(k, right, 0, Q_RA, mate).start()

    def relay_third(k):
        piece(k, opp, 0, F_R, right).wait_recv()
        piece(k, opp, 0, Q_OA, mate).start()
        piece(k, opp, 1, F_L, left).wait_recv()
        piece(k, opp, 1, Q_OB, mate).start()

    def drain(k):
        src, dst = gathers[k]
        for i in (R_A, R_B, L_A, L_B, F_R, F_L, Q_LA, Q_LB, Q_RA, Q_RB, Q_OA, Q_OB):
            piece(k, me, 0, i, right).wait_send()
        remote(src, dst.at[whole(me)], k, Q_OWN, mate).wait_send()

    def wait_mate(k, *slots):
        for i in slots:
            piece(k, me, 0, i, mate).wait_recv()

    def own_from_mate(k):
        src, dst = gathers[k]
        remote(src, dst.at[whole(me)], k, Q_OWN, mate).wait_recv()

    barrier = pltpu.get_barrier_semaphore()
    for dev in (right, left, mate):
        pl.semaphore_signal(barrier, inc=1, device_id={"tp": dev}, device_id_type=MESH)
    pl.semaphore_wait(barrier, 3)
    send_own(0)

    chips = (me, left, right, opp)

    def device(j, slot):
        return chips[j] if slot == 1 else chips[j] + 1 - 2 * core

    def u_load(j, slot):
        return (
            pltpu.make_async_copy(ug.at[whole(device(j, slot))], vug.at[slot], usem.at[0, slot]),
            pltpu.make_async_copy(uu.at[whole(device(j, slot))], vuu.at[slot], usem.at[1, slot]),
        )

    def y_load(j, slot):
        i = 2 * (j % 2) + slot
        src = dy if j == 0 and slot == 1 else dyg.at[whole(device(j, slot))]
        return pltpu.make_async_copy(src, vdy.at[at(i)], dsem.at[i])

    def outs(j, slot):
        d = device(j, slot)
        return (
            pltpu.make_async_copy(vdug.at[slot], dug.at[whole(d)], osem.at[0, slot]),
            pltpu.make_async_copy(vduu.at[slot], duu.at[whole(d)], osem.at[1, slot]),
        )

    def p_out(j):
        if j == 0:
            return (pltpu.make_async_copy(vp.at[1], s_own, psem.at[0]),)
        dst = ((s_la, s_lb0, s_lb), (s_ra0, s_ra, s_rb), (s_oa, s_ob))[j - 1]
        copies, r = [], 0
        for i, o in enumerate(dst):
            copies.append(pltpu.make_async_copy(vp.at[1, pl.ds(r, o.shape[0])], o, psem.at[i]))
            r += o.shape[0]
        return copies

    def swap(j):
        return send(vp.at[0], vq.at[j % 2], sx.at[j], rx.at[j], mate)

    def start(copies):
        for c in copies:
            c.start()

    def wait(copies):
        for c in copies:
            c.wait()

    load_wd = pltpu.make_async_copy(wd, vwd, wsem.at[0])
    load_w = (pltpu.make_async_copy(wg, vwg, wsem.at[1]), pltpu.make_async_copy(wu, vwu, wsem.at[2]))
    own_x = (pltpu.make_async_copy(x, vdy.at[at(2)], dsem.at[2]), pltpu.make_async_copy(vdy.at[at(2)], xg.at[whole(me)], qsem.at[0]))
    y_load(0, 1).start()
    start(u_load(0, 1))
    load_wd.start()
    start(u_load(0, 0))
    start(load_w)
    own_x[0].start()

    gn, hn, nt = min(512, ff), min(1024, hid), min(512, hid)

    def gate(j, slot):
        y_load(j, slot).wait()
        wait(u_load(j, slot))
        if j > 0:
            wait(outs(j - 1, slot))

        @pl.loop(0, ff // gn)
        def _(i):
            cols = pl.ds(pl.multiple_of(i * gn, gn), gn)
            y = vdy[at(2 * (j % 2) + slot), :]
            g = lax.dot_general(y, vwd[cols, :], NT, preferred_element_type=F32)
            u = vug[slot, :, cols].astype(F32)
            v = vuu[slot, :, cols].astype(F32)
            s = jax.nn.sigmoid(u)
            a = u * s
            vz[at(slot), cols] = (a * v).astype(BF)
            vduu[slot, :, cols] = (g * a).astype(BF)
            vdug[slot, :, cols] = (g * v * s * (1.0 + u * (1.0 - s))).astype(BF)

        start(outs(j, slot))
        if j < 3:
            start(u_load(j + 1, slot))

    def partial(j, slot):
        @pl.loop(0, hid // hn)
        def _(i):
            cols = pl.ds(pl.multiple_of(i * hn, hn), hn)
            p = lax.dot_general(vdug[slot], vwg[cols, :], NT, preferred_element_type=F32)
            p += lax.dot_general(vduu[slot], vwu[cols, :], NT, preferred_element_type=F32)
            if slot == 1:
                p += vq[j % 2, :, cols].astype(F32)
            vp[slot, :, cols] = p.astype(BF)

    def down(j):
        base = 2 * rows * (j % 2)

        @pl.loop(0, ff // gn)
        def _(i):
            mine = pl.ds(pl.multiple_of(i * gn, gn), gn)
            zt = vz[:, mine]
            for k in range(0, hid, nt):
                y = vdy[pl.ds(base, 2 * rows), k : k + nt]
                q = lax.dot_general(zt, y, TN, preferred_element_type=F32)
                if j == 0:
                    vdw[mine, k : k + nt] = q
                else:
                    vdw[mine, k : k + nt] += q

    def chip(j, before_mate=None, before_down=None):
        gate(j, 1)
        if before_mate is not None:
            before_mate()
        gate(j, 0)
        if j == 0:
            wait(load_w)
        else:
            swap(j - 1).wait_send()
        partial(j, 0)
        swap(j).start()
        if before_down is not None:
            before_down()
        down(j)
        swap(j).wait_recv()
        if j > 0:
            wait(p_out(j - 1))
        partial(j, 1)
        start(p_out(j))

    def first_mate():
        own_from_mate(0)
        y_load(0, 0).start()
        own_x[0].wait()
        own_x[1].start()

    load_wd.wait()
    chip(0, before_mate=first_mate)
    own_x[1].wait()
    relay_first(0)
    send_own(1)
    relay_second(0)
    y_load(1, 1).start()
    wait_mate(0, Q_LA, Q_LB)
    y_load(1, 0).start()

    def fetch_right():
        y_load(2, 1).start()
        wait_mate(0, Q_RA, Q_RB)
        y_load(2, 0).start()

    chip(1, before_down=fetch_right)
    relay_third(0)

    def fetch_opp():
        y_load(3, 1).start()
        wait_mate(0, Q_OA, Q_OB)
        y_load(3, 0).start()

    chip(2, before_down=fetch_opp)
    relay_first(1)
    chip(3)
    dw_out = pltpu.make_async_copy(vdw, dwd, qsem.at[0])
    dw_out.start()
    near = (send(s_ra0, got_a, se.at[0], re.at[0], right), send(s_lb0, got_b, se.at[1], re.at[1], left))
    start(near)
    relay_second(1)
    relay_third(1)
    for slot in (0, 1):
        wait(outs(3, slot))
    wait(p_out(3))
    swap(3).wait_send()
    dw_out.wait()
    own_from_mate(1)
    wait_mate(1, Q_LA, Q_LB, Q_RA, Q_RB, Q_OA, Q_OB)
    wait(near)
    drain(0)
    drain(1)


def gather_and_local(n, x, dy, wd, wg, wu, ug, uu):
    rows, hid = x.shape
    tok, ff = ug.shape
    half = rows // 2
    early = half // EARLY
    any_ = pl.BlockSpec(memory_space=pl.ANY)
    sds = jax.ShapeDtypeStruct

    def r(k):
        return sds((k, hid), BF)

    out = [r(tok), r(tok), sds((tok, ff), BF), sds((tok, ff), BF), sds((ff, hid), F32), r(rows)]
    out += [r(half), r(early), r(half - early), r(early), r(half - early), r(half), r(half), r(half), r(early), r(early)]
    return pl.pallas_call(
        functools.partial(gather_kernel, n),
        out_shape=out,
        in_specs=[any_] * 7,
        out_specs=[any_] * len(out),
        scratch_shapes=[
            pltpu.VMEM(wd.shape, BF), pltpu.VMEM(wg.shape, BF), pltpu.VMEM(wu.shape, BF),
            pltpu.VMEM((4 * rows, hid), BF),
            pltpu.VMEM((2, rows, ff), BF), pltpu.VMEM((2, rows, ff), BF),
            pltpu.VMEM((2, rows, ff), BF), pltpu.VMEM((2, rows, ff), BF), pltpu.VMEM((2 * rows, ff), BF),
            pltpu.VMEM((2, rows, hid), BF),
            pltpu.VMEM((2, rows, hid), BF),
            pltpu.VMEM((ff, hid), F32),
            pltpu.SemaphoreType.DMA((2, 13)), pltpu.SemaphoreType.DMA((2, 13)),
            pltpu.SemaphoreType.DMA((4,)), pltpu.SemaphoreType.DMA((4,)),
            pltpu.SemaphoreType.DMA((2,)), pltpu.SemaphoreType.DMA((2,)),
            pltpu.SemaphoreType.DMA((3,)), pltpu.SemaphoreType.DMA((2, 2)), pltpu.SemaphoreType.DMA((4,)),
            pltpu.SemaphoreType.DMA((2, 2)), pltpu.SemaphoreType.DMA((3,)), pltpu.SemaphoreType.DMA((2,)),
        ],
        compiler_params=pltpu.CompilerParams(collective_id=0, has_side_effects=True, vmem_limit_bytes=62 * 2**20),
        cost_estimate=pl.CostEstimate(flops=8 * tok * hid * ff, bytes_accessed=100 * 2**20, transcendentals=tok * ff),
    )(x, dy, wd, wg, wu, ug, uu)


def tokens_kernel(kt, a, b, *refs):
    *thru, vb, sem = refs
    if len(thru) == 3:
        spare, o, spare_out = thru
        spare_out[...] = spare[...]
    else:
        (o,) = thru
    tok = a.shape[0]
    copies = [
        pltpu.make_async_copy(b.at[pl.ds(k, kt)], vb.at[pl.ds(k, kt)], sem.at[k // kt]) for k in range(0, tok, kt)
    ]

    @pl.when(pl.program_id(0) == 0)
    def _():
        for c in copies:
            c.start()
        for i, c in enumerate(copies):
            c.wait()
            ks = pl.ds(i * kt, kt)
            p = lax.dot_general(a[ks, :], vb[ks, :], TN, preferred_element_type=F32)
            if i == 0:
                o[...] = p
            else:
                o[...] += p

    @pl.when(pl.program_id(0) > 0)
    def _():
        o[...] = lax.dot_general(a[...], vb[...], TN, preferred_element_type=F32)


def over_tokens(a, b, spare=None, m_tile=256, kt=768):
    tok, m = a.shape
    k = b.shape[1]
    m_tile, kt = min(m_tile, m), min(kt, tok)
    steps = m // m_tile
    out_shape = [jax.ShapeDtypeStruct((m, k), F32)]
    in_specs = [pl.BlockSpec((tok, m_tile), lambda i: (0, i)), pl.BlockSpec(memory_space=pl.ANY)]
    out_specs = [pl.BlockSpec((m_tile, k), lambda i: (i, 0))]
    args = [a, b]
    if spare is not None:
        block = pl.BlockSpec((spare.shape[0] // steps, spare.shape[1]), lambda i: (i, 0))
        out_shape.append(jax.ShapeDtypeStruct(spare.shape, spare.dtype))
        in_specs.append(block)
        out_specs.append(block)
        args.append(spare)
    return pl.pallas_call(
        functools.partial(tokens_kernel, kt),
        grid=(steps,),
        out_shape=out_shape,
        in_specs=in_specs,
        out_specs=out_specs,
        scratch_shapes=[pltpu.VMEM((tok, k), BF), pltpu.SemaphoreType.DMA((tok // kt,))],
        compiler_params=pltpu.CompilerParams(vmem_limit_bytes=62 * 2**20),
        cost_estimate=pl.CostEstimate(
            flops=2 * tok * m * k, bytes_accessed=2 * tok * (m + k) + 4 * m * k, transcendentals=0
        ),
    )(*args)


def pair_kernel(a, b, c, d, ab, cd):
    ab[...] = (a[...].astype(F32) + b[...].astype(F32)).astype(BF)
    cd[...] = (c[...].astype(F32) + d[...].astype(F32)).astype(BF)


def pair_sum(a, b, c, d, steps=2):
    rows, hid = a.shape
    block = pl.BlockSpec((rows // steps, hid), lambda i: (i, 0))
    return pl.pallas_call(
        pair_kernel,
        grid=(steps,),
        out_shape=[jax.ShapeDtypeStruct(a.shape, BF)] * 2,
        in_specs=[block] * 4,
        out_specs=[block] * 2,
        compiler_params=pltpu.CompilerParams(vmem_limit_bytes=16 * 2**20),
        cost_estimate=pl.CostEstimate(flops=2 * rows * hid, bytes_accessed=12 * rows * hid, transcendentals=0),
    )(a, b, c, d)


def final_kernel(own, got_a, got_b, near_a, near_b, far_a, far_b, o):
    first = pl.program_id(0) == 0
    for i, (got, near, far) in enumerate(((got_a, near_a, far_a), (got_b, near_b, far_b))):
        direct = jnp.where(first, got[...], near[...]).astype(F32)
        o[i] = (own[i].astype(F32) + direct + far[...].astype(F32)).astype(BF)


def final_sum(own, got_a, got_b, near_a, near_b, far_a, far_b):
    rows, hid = own.shape
    half = rows // 2
    t = got_a.shape[0]
    both = pl.BlockSpec((2, t, hid), lambda i: (0, i, 0))
    one = pl.BlockSpec((t, hid), lambda i: (i, 0))
    got = pl.BlockSpec((t, hid), lambda i: (0, 0))
    near = pl.BlockSpec((t, hid), lambda i: (jnp.maximum(i - 1, 0), 0))
    return pl.pallas_call(
        final_kernel,
        grid=(half // t,),
        out_shape=jax.ShapeDtypeStruct((2, half, hid), BF),
        in_specs=[both, got, got, near, near, one, one],
        out_specs=both,
        compiler_params=pltpu.CompilerParams(vmem_limit_bytes=16 * 2**20),
        cost_estimate=pl.CostEstimate(flops=rows * hid * 3, bytes_accessed=8 * rows * hid, transcendentals=0),
    )(own.reshape(2, half, hid), got_a, got_b, near_a, near_b, far_a, far_b).reshape(rows, hid)


def solution(mesh):
    tok = P(("dp", "tp"), None)
    col = P(None, "tp")
    row = P("tp", None)
    act = P("dp", "tp")
    n = mesh.shape["tp"]
    to_right = [(i, (i + 2) % n) for i in range(n)]
    to_left = [(i, (i - 2) % n) for i in range(n)]

    def body(x, dy, wg, wu, wd, ug, uu):
        xg, _, dug, duu, dwd, s_own, s_la, _, s_lb, _, s_ra, s_rb, s_oa, s_ob, got_a, got_b = (
            gather_and_local(n, x, dy, wd, wg, wu, ug, uu)
        )

        def right(v):
            return lax.ppermute(v, "tp", to_right)

        def left(v):
            return lax.ppermute(v, "tp", to_left)

        from_right = left(s_oa)
        from_left = right(s_ob)
        direct_a = right(s_ra)
        direct_b = left(s_lb)
        (dwg,) = over_tokens(xg, dug)
        from_right, from_left, dwg = lax.optimization_barrier((from_right, from_left, dwg))
        next_l, next_r = pair_sum(s_la, from_right, s_rb, from_left)
        next_l, next_r, xg = lax.optimization_barrier((next_l, next_r, xg))
        relay_a = left(next_l)
        relay_b = right(next_r)
        dwu, dwd = over_tokens(xg, duu, spare=dwd)
        dx = final_sum(s_own, got_a, got_b, direct_a, direct_b, relay_a, relay_b)
        return dx, dwg, dwu, dwd

    return jax.shard_map(
        body, mesh=mesh, in_specs=(tok, tok, col, col, row, act, act), out_specs=(tok, act, act, tok), check_vma=False
    )
```

```python
import functools

import jax
import jax.numpy as jnp
from jax import lax
from jax.experimental import pallas as pl
from jax.experimental.pallas import tpu as pltpu
from jax.sharding import PartitionSpec as P


MESH = pl.DeviceIdType.MESH
BF = jnp.bfloat16
F32 = jnp.float32
NT = (((1,), (1,)), ((), ()))
TN = (((0,), (0,)), ((), ()))

EARLY = 3

R_A, R_B, L_A, L_B, F_R, F_L, Q_OWN, Q_LA, Q_LB, Q_RA, Q_RB, Q_OA, Q_OB = range(13)
LEFT, RIGHT, OPP, OWN = range(4)


def gather_kernel(
    n, x, dy, wd, wg, wu, ug, uu,
    xg, dyg, dug, duu, dwd, part_g, part_u, s_own, s_la, s_lb0, s_lb, s_ra0, s_ra, s_rb, s_oa, s_ob, got_a, got_b,
    vwd, vwg, vwu, vdy, vug, vuu, vdug, vduu, vz, vp, vq, vdw, vt,
    ss, rs, sx, rx, se, re, wsem, usem, dsem, osem, psem, qsem, tsem,
):
    rows, hid = x.shape
    half = rows // 2
    ff = wd.shape[0]
    me = lax.axis_index("tp")
    core = lax.rem(me, 2)
    right, left = lax.rem(me + 2, n), lax.rem(me + n - 2, n)
    opp = lax.rem(me + 4, n)
    mate = me + 1 - 2 * core

    def whole(d):
        return pl.ds(pl.multiple_of(d * rows, rows), rows)

    def pos(rel, c):
        return pl.ds(pl.multiple_of((2 * rel + c) * rows, rows), rows)

    def part(rel, h):
        return pl.ds(pl.multiple_of((2 * rel + core) * rows + h * half, half), half)

    def at(slot):
        return pl.ds(slot * rows, rows)

    def send(src, dst, s_sem, r_sem, dev):
        return pltpu.make_async_remote_copy(
            src, dst, s_sem, r_sem, device_id={"tp": dev}, device_id_type=MESH
        )

    def remote(src, dst, k, i, dev):
        return send(src, dst, ss.at[k, i], rs.at[k, i], dev)

    gathers = ((dy, dyg), (x, xg))

    def send_own(k):
        src, dst = gathers[k]
        a, b = pl.ds(0, half), pl.ds(half, half)
        remote(src.at[a], dst.at[part(LEFT, 0)], k, R_A, right).start()
        remote(src.at[b], dst.at[part(RIGHT, 1)], k, L_B, left).start()
        remote(src.at[b], dst.at[part(LEFT, 1)], k, R_B, right).start()
        remote(src.at[a], dst.at[part(RIGHT, 0)], k, L_A, left).start()

    def own_to_mate(k):
        src, dst = gathers[k]
        return remote(src, dst.at[pos(OWN, core)], k, Q_OWN, mate)

    def piece(k, rel, h, i, dev, to=None):
        dst = gathers[k][1]
        return remote(dst.at[part(rel, h)], dst.at[part(rel if to is None else to, h)], k, i, dev)

    def relay_first(k):
        piece(k, LEFT, 0, R_A, right).wait_recv()
        piece(k, LEFT, 0, F_R, right, OPP).start()
        piece(k, LEFT, 0, Q_LA, mate).start()
        piece(k, RIGHT, 1, L_B, left).wait_recv()
        piece(k, RIGHT, 1, F_L, left, OPP).start()
        piece(k, RIGHT, 1, Q_RB, mate).start()

    def relay_second(k):
        piece(k, LEFT, 1, R_B, right).wait_recv()
        piece(k, LEFT, 1, Q_LB, mate).start()
        piece(k, RIGHT, 0, L_A, left).wait_recv()
        piece(k, RIGHT, 0, Q_RA, mate).start()

    def relay_third(k):
        piece(k, OPP, 0, F_R, right).wait_recv()
        piece(k, OPP, 0, Q_OA, mate).start()
        piece(k, OPP, 1, F_L, left).wait_recv()
        piece(k, OPP, 1, Q_OB, mate).start()

    def drain(k):
        for i in (R_A, R_B, L_A, L_B, F_R, F_L, Q_LA, Q_LB, Q_RA, Q_RB, Q_OA, Q_OB):
            piece(k, OWN, 0, i, right).wait_send()
        own_to_mate(k).wait_send()

    def wait_mate(k, *slots):
        for i in slots:
            piece(k, OWN, 0, i, mate).wait_recv()

    barrier = pltpu.get_barrier_semaphore()
    for dev in (right, left, mate):
        pl.semaphore_signal(barrier, inc=1, device_id={"tp": dev}, device_id_type=MESH)
    pl.semaphore_wait(barrier, 3)
    own_to_mate(0).start()
    send_own(0)
    own_to_mate(1).start()

    chips = (me, left, right, opp)

    def device(j, slot):
        return chips[j] if slot == 1 else chips[j] + 1 - 2 * core

    places = (OWN, LEFT, RIGHT, OPP)

    def place(j, slot):
        return pos(places[j], core if slot == 1 else 1 - core)

    def u_load(j, slot):
        return (
            pltpu.make_async_copy(ug.at[whole(device(j, slot))], vug.at[slot], usem.at[0, slot]),
            pltpu.make_async_copy(uu.at[whole(device(j, slot))], vuu.at[slot], usem.at[1, slot]),
        )

    def y_load(j, slot):
        i = 2 * (j % 2) + slot
        src = dy if j == 0 and slot == 1 else dyg.at[place(j, slot)]
        return pltpu.make_async_copy(src, vdy.at[at(i)], dsem.at[i])

    def outs(j, slot):
        return (
            pltpu.make_async_copy(vdug.at[slot], dug.at[place(j, slot)], osem.at[0, slot]),
            pltpu.make_async_copy(vduu.at[slot], duu.at[place(j, slot)], osem.at[1, slot]),
        )

    def p_out(j):
        if j == 0:
            return (pltpu.make_async_copy(vp.at[1], s_own, psem.at[0]),)
        dst = ((s_la, s_lb0, s_lb), (s_ra0, s_ra, s_rb), (s_oa, s_ob))[j - 1]
        copies, r = [], 0
        for i, o in enumerate(dst):
            copies.append(pltpu.make_async_copy(vp.at[1, pl.ds(r, o.shape[0])], o, psem.at[i]))
            r += o.shape[0]
        return copies

    def swap(j):
        return send(vp.at[0], vq.at[j % 2], sx.at[j], rx.at[j], mate)

    def start(copies):
        for c in copies:
            c.start()

    def wait(copies):
        for c in copies:
            c.wait()

    load_wd = pltpu.make_async_copy(wd, vwd, wsem.at[0])
    load_w = (pltpu.make_async_copy(wg, vwg, wsem.at[1]), pltpu.make_async_copy(wu, vwu, wsem.at[2]))
    own_x = pltpu.make_async_copy(x, vdy.at[at(3)], dsem.at[3])
    mate_x = pltpu.make_async_copy(xg.at[pos(OWN, 1 - core)], vdy.at[at(2)], dsem.at[2])
    y_load(0, 1).start()
    start(u_load(0, 1))
    load_wd.start()
    start(u_load(0, 0))
    start(load_w)
    own_x.start()

    gn, hn, nt = min(512, ff), min(1024, hid), min(512, hid)

    def gate(j, slot):
        y_load(j, slot).wait()
        wait(u_load(j, slot))
        if j > 0:
            wait(outs(j - 1, slot))

        @pl.loop(0, ff // gn)
        def _(i):
            cols = pl.ds(pl.multiple_of(i * gn, gn), gn)
            y = vdy[at(2 * (j % 2) + slot), :]
            g = lax.dot_general(y, vwd[cols, :], NT, preferred_element_type=F32)
            u = vug[slot, :, cols].astype(F32)
            v = vuu[slot, :, cols].astype(F32)
            s = jax.nn.sigmoid(u)
            a = u * s
            vz[at(slot), cols] = (a * v).astype(BF)
            vduu[slot, :, cols] = (g * a).astype(BF)
            vdug[slot, :, cols] = (g * v * s * (1.0 + u * (1.0 - s))).astype(BF)

        start(outs(j, slot))
        if j < 3:
            start(u_load(j + 1, slot))

    def partial(j, slot):
        @pl.loop(0, hid // hn)
        def _(i):
            cols = pl.ds(pl.multiple_of(i * hn, hn), hn)
            p = lax.dot_general(vdug[slot], vwg[cols, :], NT, preferred_element_type=F32)
            p += lax.dot_general(vduu[slot], vwu[cols, :], NT, preferred_element_type=F32)
            if slot == 1:
                p += vq[j % 2, :, cols].astype(F32)
            vp[slot, :, cols] = p.astype(BF)

    def down(j):
        base = 2 * rows * (j % 2)

        @pl.loop(0, ff // gn)
        def _(i):
            mine = pl.ds(pl.multiple_of(i * gn, gn), gn)
            zt = vz[:, mine]
            for k in range(0, hid, nt):
                y = vdy[pl.ds(base, 2 * rows), k : k + nt]
                q = lax.dot_general(zt, y, TN, preferred_element_type=F32)
                if j == 0:
                    vdw[mine, k : k + nt] = q
                else:
                    vdw[mine, k : k + nt] += q

    def chip(j, before_mate=None, before_down=None):
        gate(j, 1)
        if before_mate is not None:
            before_mate()
        gate(j, 0)
        if j == 0:
            wait(load_w)
        else:
            swap(j - 1).wait_send()
        partial(j, 0)
        swap(j).start()
        if before_down is not None:
            before_down()
        down(j)
        swap(j).wait_recv()
        if j > 0:
            wait(p_out(j - 1))
        partial(j, 1)
        start(p_out(j))

    def first_mate():
        own_to_mate(0).wait_recv()
        y_load(0, 0).start()

    def first_down():
        own_to_mate(1).wait_recv()
        mate_x.start()

    def own_tokens():
        mt = vt.shape[1]
        for src, out in ((vdug, part_g), (vduu, part_u)):

            def leave(r, i):
                return pltpu.make_async_copy(vt.at[i], out.at[pl.ds(pl.multiple_of(r, mt), mt)], tsem.at[i])

            @pl.loop(0, hid // (2 * mt))
            def _(t):
                for i in (0, 1):
                    r = (2 * t + i) * mt

                    @pl.when(t > 0)
                    def _():
                        leave(r, i).wait()

                    xt = vdy[pl.ds(2 * rows, 2 * rows), pl.ds(pl.multiple_of(r, mt), mt)]
                    vt[i] = lax.dot_general(xt, src[...].reshape(2 * rows, ff), TN, preferred_element_type=F32)
                    leave(r, i).start()

            for i in (0, 1):
                leave(i * mt, i).wait()

    load_wd.wait()
    chip(0, before_mate=first_mate, before_down=first_down)
    relay_first(0)
    send_own(1)
    own_x.wait()
    mate_x.wait()
    own_tokens()
    relay_second(0)
    y_load(1, 1).start()
    wait_mate(0, Q_LA, Q_LB)
    y_load(1, 0).start()

    def fetch_right():
        y_load(2, 1).start()
        wait_mate(0, Q_RA, Q_RB)
        y_load(2, 0).start()

    chip(1, before_down=fetch_right)
    relay_third(0)

    def fetch_opp():
        y_load(3, 1).start()
        wait_mate(0, Q_OA, Q_OB)
        y_load(3, 0).start()

    chip(2, before_down=fetch_opp)
    relay_first(1)
    chip(3)
    dw_out = pltpu.make_async_copy(vdw, dwd, qsem.at[0])
    dw_out.start()
    near = (send(s_ra0, got_a, se.at[0], re.at[0], right), send(s_lb0, got_b, se.at[1], re.at[1], left))
    start(near)
    relay_second(1)
    relay_third(1)
    for slot in (0, 1):
        wait(outs(3, slot))
    wait(p_out(3))
    swap(3).wait_send()
    dw_out.wait()
    wait_mate(1, Q_LA, Q_LB, Q_RA, Q_RB, Q_OA, Q_OB)
    wait(near)
    drain(0)
    drain(1)


def gather_and_local(n, x, dy, wd, wg, wu, ug, uu):
    rows, hid = x.shape
    tok, ff = ug.shape
    half = rows // 2
    early = half // EARLY
    any_ = pl.BlockSpec(memory_space=pl.ANY)
    sds = jax.ShapeDtypeStruct

    def r(k):
        return sds((k, hid), BF)

    out = [r(tok), r(tok), sds((tok, ff), BF), sds((tok, ff), BF), sds((ff, hid), F32)]
    out += [sds((hid, ff), F32), sds((hid, ff), F32), r(rows)]
    out += [r(half), r(early), r(half - early), r(early), r(half - early), r(half), r(half), r(half), r(early), r(early)]
    return pl.pallas_call(
        functools.partial(gather_kernel, n),
        out_shape=out,
        in_specs=[any_] * 7,
        out_specs=[any_] * len(out),
        scratch_shapes=[
            pltpu.VMEM(wd.shape, BF), pltpu.VMEM(wg.shape, BF), pltpu.VMEM(wu.shape, BF),
            pltpu.VMEM((4 * rows, hid), BF),
            pltpu.VMEM((2, rows, ff), BF), pltpu.VMEM((2, rows, ff), BF),
            pltpu.VMEM((2, rows, ff), BF), pltpu.VMEM((2, rows, ff), BF), pltpu.VMEM((2 * rows, ff), BF),
            pltpu.VMEM((2, rows, hid), BF),
            pltpu.VMEM((2, rows, hid), BF),
            pltpu.VMEM((ff, hid), F32),
            pltpu.VMEM((2, min(256, hid), ff), F32),
            pltpu.SemaphoreType.DMA((2, 13)), pltpu.SemaphoreType.DMA((2, 13)),
            pltpu.SemaphoreType.DMA((4,)), pltpu.SemaphoreType.DMA((4,)),
            pltpu.SemaphoreType.DMA((2,)), pltpu.SemaphoreType.DMA((2,)),
            pltpu.SemaphoreType.DMA((3,)), pltpu.SemaphoreType.DMA((2, 2)), pltpu.SemaphoreType.DMA((4,)),
            pltpu.SemaphoreType.DMA((2, 2)), pltpu.SemaphoreType.DMA((3,)), pltpu.SemaphoreType.DMA((2,)), pltpu.SemaphoreType.DMA((2,)),
        ],
        compiler_params=pltpu.CompilerParams(collective_id=0, has_side_effects=True, vmem_limit_bytes=62 * 2**20),
        cost_estimate=pl.CostEstimate(flops=8 * tok * hid * ff, bytes_accessed=100 * 2**20, transcendentals=tok * ff),
    )(x, dy, wd, wg, wu, ug, uu)


def tokens_kernel(a, b, init, *refs):
    if len(refs) == 3:
        spare, o, spare_out = refs
        spare_out[...] = spare[...]
    else:
        (o,) = refs
    o[...] = init[...] + lax.dot_general(a[...], b[...], TN, preferred_element_type=F32)


def over_tokens(a, b, init, spare=None, m_tile=512):
    m = a.shape[1]
    tok = a.shape[0] // 4 * 3
    k = b.shape[1]
    m_tile = min(m_tile, m)
    steps = m // m_tile
    tile = pl.BlockSpec((m_tile, k), lambda i: (i, 0))
    whole = pl.BlockSpec((tok, k), lambda i: (0, 0), pipeline_mode=pl.Buffered(1))
    out_shape = [jax.ShapeDtypeStruct((m, k), F32)]
    in_specs = [pl.BlockSpec((tok, m_tile), lambda i: (0, i)), whole, tile]
    out_specs = [tile]
    args = [a, b, init]
    if spare is not None:
        block = pl.BlockSpec((spare.shape[0] // steps, spare.shape[1]), lambda i: (i, 0))
        out_shape.append(jax.ShapeDtypeStruct(spare.shape, spare.dtype))
        in_specs.append(block)
        out_specs.append(block)
        args.append(spare)
    return pl.pallas_call(
        tokens_kernel,
        grid=(steps,),
        out_shape=out_shape,
        in_specs=in_specs,
        out_specs=out_specs,
        compiler_params=pltpu.CompilerParams(vmem_limit_bytes=36 * 2**20),
        cost_estimate=pl.CostEstimate(
            flops=2 * tok * m * k, bytes_accessed=2 * tok * (m + k) + 8 * m * k, transcendentals=0
        ),
    )(*args)


def pair_kernel(a, b, c, d, ab, cd):
    ab[...] = (a[...].astype(F32) + b[...].astype(F32)).astype(BF)
    cd[...] = (c[...].astype(F32) + d[...].astype(F32)).astype(BF)


def pair_sum(a, b, c, d, steps=2):
    rows, hid = a.shape
    block = pl.BlockSpec((rows // steps, hid), lambda i: (i, 0))
    return pl.pallas_call(
        pair_kernel,
        grid=(steps,),
        out_shape=[jax.ShapeDtypeStruct(a.shape, BF)] * 2,
        in_specs=[block] * 4,
        out_specs=[block] * 2,
        compiler_params=pltpu.CompilerParams(vmem_limit_bytes=16 * 2**20),
        cost_estimate=pl.CostEstimate(flops=2 * rows * hid, bytes_accessed=12 * rows * hid, transcendentals=0),
    )(a, b, c, d)


def final_kernel(own, got_a, got_b, near_a, near_b, far_a, far_b, o):
    first = pl.program_id(0) == 0
    for i, (got, near, far) in enumerate(((got_a, near_a, far_a), (got_b, near_b, far_b))):
        direct = jnp.where(first, got[...], near[...]).astype(F32)
        o[i] = (own[i].astype(F32) + direct + far[...].astype(F32)).astype(BF)


def final_sum(own, got_a, got_b, near_a, near_b, far_a, far_b):
    rows, hid = own.shape
    half = rows // 2
    t = got_a.shape[0]
    both = pl.BlockSpec((2, t, hid), lambda i: (0, i, 0))
    one = pl.BlockSpec((t, hid), lambda i: (i, 0))
    got = pl.BlockSpec((t, hid), lambda i: (0, 0))
    near = pl.BlockSpec((t, hid), lambda i: (jnp.maximum(i - 1, 0), 0))
    return pl.pallas_call(
        final_kernel,
        grid=(half // t,),
        out_shape=jax.ShapeDtypeStruct((2, half, hid), BF),
        in_specs=[both, got, got, near, near, one, one],
        out_specs=both,
        compiler_params=pltpu.CompilerParams(vmem_limit_bytes=16 * 2**20),
        cost_estimate=pl.CostEstimate(flops=rows * hid * 3, bytes_accessed=8 * rows * hid, transcendentals=0),
    )(own.reshape(2, half, hid), got_a, got_b, near_a, near_b, far_a, far_b).reshape(rows, hid)


def solution(mesh):
    tok = P(("dp", "tp"), None)
    col = P(None, "tp")
    row = P("tp", None)
    act = P("dp", "tp")
    n = mesh.shape["tp"]
    to_right = [(i, (i + 2) % n) for i in range(n)]
    to_left = [(i, (i - 2) % n) for i in range(n)]

    def body(x, dy, wg, wu, wd, ug, uu):
        xg, _, dug, duu, dwd, part_g, part_u, s_own, s_la, _, s_lb, _, s_ra, s_rb, s_oa, s_ob, got_a, got_b = (
            gather_and_local(n, x, dy, wd, wg, wu, ug, uu)
        )

        def right(v):
            return lax.ppermute(v, "tp", to_right)

        def left(v):
            return lax.ppermute(v, "tp", to_left)

        from_right = left(s_oa)
        from_left = right(s_ob)
        direct_a = right(s_ra)
        direct_b = left(s_lb)
        (dwg,) = over_tokens(xg, dug, part_g)
        from_right, from_left, dwg = lax.optimization_barrier((from_right, from_left, dwg))
        next_l, next_r = pair_sum(s_la, from_right, s_rb, from_left)
        next_l, next_r, xg = lax.optimization_barrier((next_l, next_r, xg))
        relay_a = left(next_l)
        relay_b = right(next_r)
        dwu, dwd = over_tokens(xg, duu, part_u, spare=dwd)
        dx = final_sum(s_own, got_a, got_b, direct_a, direct_b, relay_a, relay_b)
        return dx, dwg, dwu, dwd

    return jax.shard_map(
        body, mesh=mesh, in_specs=(tok, tok, col, col, row, act, act), out_specs=(tok, act, act, tok), check_vma=False
    )
```
